128 devices in a mesh: dp: 4 (over z), mp: 32 (over y, x, core).
Axes of the slice: x: 4, y: 4, z: 4, core: 2. Of those that a mesh axis runs over, the one named last changes fastest.
Arguments:
- tokens: bfloat16 [4096, 4096], P('dp', 'mp'), may hold values from -6 to 6
- decay: float32 [4096, 16], P('dp'), may hold values from 0.75 to 1, as said below
- state: float32 [128, 256, 8192], P('dp', None, 'mp'), may hold values from -24 to 24
- w_query: bfloat16 [4096, 4096], P(None, 'mp'), may hold values from -0.09375 to 0.09375
- w_key: bfloat16 [4096, 4096], P(None, 'mp'), may hold values from -0.09375 to 0.09375
- w_value: bfloat16 [4096, 8192], P(None, 'mp'), may hold values from -0.09375 to 0.09375
- w_gate: bfloat16 [4096, 8192], P(None, 'mp'), may hold values from -0.09375 to 0.09375
- w_out: bfloat16 [8192, 4096], P('mp'), may hold values from -0.125 to 0.125
- norm_gain: float32 [8192], P('mp'), may hold values from 0.25 to 1.75
Outputs:
- layer_out: bfloat16 [4096, 4096], P('dp', 'mp')
- new_state: float32 [128, 256, 8192], P('dp', None, 'mp')
The draws below stay inside these ranges and needn't reach their ends.
Inputs may be any that keep to these rules, and one draw needn't show every extreme that they name: `decay`: each head has its own base rate over all tokens, varied somewhat from token to token.
All inputs are finite; a program needn't handle non-finite values.
Results may differ from the reference program's by a relative error of at most 0.0071.
Values may be sent and summed in bfloat16 or wider, within the bound.
No kernel may reach another device: no remote copies, remote signals or barrier semaphores. Data moves between devices by JAX's collectives and lax.ppermute only.
A program may use at most 128 MiB of HBM per device.

```python
import jax
import jax.numpy as jnp
from jax import lax

D = 4096
H = 16
HEAD = 256
VHEAD = 512
NEW = 32
BATCH = 128
TOKENS = 4096


def draw_decay(key, part):
    base_key, jitter_key = jax.random.split(key)
    base_low = 0.85
    jitter_low = 0.93
    base_rate = jnp.exp(jax.random.uniform(base_key, (H,), jnp.float32, jnp.log(base_low), jnp.log(0.999)))
    jitter = jax.random.uniform(jitter_key, (TOKENS, H), jnp.float32, jitter_low, 1.0)
    return base_rate[None, :] * jitter


def with_spikes(result, key, source, target, parts, factor):
    owner, partner = [(jnp.arange(result.shape[position]) // (result.shape[position] // parts)).reshape([-1 if axis == position else 1 for axis in range(result.ndim)]) for position in (source, target)]
    chosen = jax.random.permutation(key, parts)[partner]
    strong = (owner == chosen) | (owner == (partner + parts // 2) % parts)
    return jnp.where(strong, factor * result, result)


def block_levels(rng, dims, shards, low, largest):
    level = 1.0
    for position, shards_of in shards:
        heights = jax.random.uniform(jax.random.fold_in(jax.random.fold_in(rng, 6), position), (shards_of,), jnp.float32, low / len(shards), largest / len(shards))
        level = level * jnp.repeat(jnp.exp(heights), dims[position] // shards_of).reshape((-1,) + (1,) * (len(dims) - 1 - position))
    return level


def gaussian(rng, shape, scale, most, cuts=(), held_as=jnp.bfloat16):
    values = scale * jax.random.normal(rng, shape, jnp.float32)
    if cuts:
        values = values * block_levels(rng, shape, cuts, -0.22, 0.18)
    return jnp.clip(values, -most, most).astype(held_as)


def bell_draw_with(own_key, shape, width, most, pieces, heavy, held_as=jnp.bfloat16):
    result = width * jax.random.normal(own_key, shape, jnp.float32)
    if pieces:
        result = result * block_levels(own_key, shape, pieces, -0.22, 0.18)
    return jnp.clip(with_spikes(result, jax.random.fold_in(own_key, 3), *heavy), -most, most).astype(held_as)


def setup_inputs(seed: int = 0) -> dict:
    arg_keys = jax.random.split(jax.random.key(seed), 10)
    return {
        "tokens": gaussian(arg_keys[0], (TOKENS, D), 1.0, 6.0, ((0, 4), (1, 32))),
        "decay": draw_decay(jax.random.fold_in(arg_keys[9], 71), 0),
        "state": gaussian(arg_keys[2], (BATCH, HEAD, H * VHEAD), 4.0, 24.0, ((0, 4), (2, 32)), jnp.float32),
        "w_query": gaussian(arg_keys[3], (D, H * HEAD), D ** -0.5, 0.09375, ((1, 32),)),
        "w_key": gaussian(arg_keys[4], (D, H * HEAD), D ** -0.5, 0.09375, ((1, 32),)),
        "w_value": gaussian(arg_keys[5], (D, H * VHEAD), D ** -0.5, 0.09375, ((1, 32),)),
        "w_gate": gaussian(arg_keys[6], (D, H * VHEAD), D ** -0.5, 0.09375, ((1, 32),)),
        "w_out": bell_draw_with(arg_keys[7], (H * VHEAD, D), (H * VHEAD) ** -0.5, 0.125, ((0, 32),), (0, 1, 32, 2.75)),
        "norm_gain": jnp.clip(1.0 + 0.15 * jax.random.normal(arg_keys[8], (H * VHEAD,), jnp.float32), 0.25, 1.75),
    }


EPS = 0.1

def one_sequence(packed):
    query, key_proj, value_proj, decay_rates, old_state = packed
    highest = lax.Precision.HIGHEST
    log_cumul = jnp.cumsum(jnp.log(decay_rates), axis=0)
    from_state = jnp.einsum('nhk,khv->nhv', query.astype(jnp.float32), old_state, precision=highest)
    scores = jnp.einsum('nhk,mhk->hnm', query.astype(jnp.float32), key_proj.astype(jnp.float32), precision=highest)
    along = log_cumul.T
    log_gap = along[:, :, None] - along[:, None, :]
    causal = jnp.arange(NEW)[:, None] >= jnp.arange(NEW)[None, :]
    factor = jnp.where(causal, jnp.exp(jnp.where(causal, log_gap, 0.0)), 0.0)
    weights = (scores * factor).astype(jnp.bfloat16)
    in_block = jnp.einsum('hnm,mhv->nhv', weights.astype(jnp.float32), value_proj.astype(jnp.float32), precision=highest)
    retained = jnp.exp(log_cumul)[:, :, None] * from_state + in_block
    final_log = log_cumul[-1]
    carry_scale = jnp.exp(final_log[None, :] - log_cumul)
    decayed_keys = key_proj.astype(jnp.float32) * carry_scale[:, :, None]
    fresh = jnp.einsum('nhk,nhv->khv', decayed_keys, value_proj.astype(jnp.float32), precision=highest)
    new_state = jnp.exp(final_log)[None, :, None] * old_state + fresh
    return (retained, new_state)

def reference(tokens, decay, state, w_query, w_key, w_value, w_gate, w_out, norm_gain):
    query = (jnp.dot(tokens, w_query, preferred_element_type=jnp.float32) * HEAD ** (-0.5)).astype(jnp.bfloat16)
    key_proj = jnp.dot(tokens, w_key, preferred_element_type=jnp.float32).astype(jnp.bfloat16)
    value_proj = jnp.dot(tokens, w_value, preferred_element_type=jnp.float32).astype(jnp.bfloat16)
    gate_proj = jnp.dot(tokens, w_gate, preferred_element_type=jnp.float32)
    packed = (query.reshape(BATCH, NEW, H, HEAD), key_proj.reshape(BATCH, NEW, H, HEAD), value_proj.reshape(BATCH, NEW, H, VHEAD), decay.reshape(BATCH, NEW, H), state.reshape(BATCH, HEAD, H, VHEAD))
    retained, new_state = lax.map(one_sequence, packed)
    retained = retained.reshape(TOKENS, H, VHEAD)
    centre = lax.optimization_barrier(jnp.mean(retained, axis=-1))
    deviation = retained - centre[..., None]
    variance = lax.optimization_barrier(jnp.mean(deviation * deviation, axis=-1))
    normed = deviation * lax.rsqrt(variance + EPS)[..., None]
    gated_out = (normed.reshape(TOKENS, H * VHEAD) * norm_gain * jax.nn.silu(gate_proj)).astype(jnp.bfloat16)
    layer_out = jnp.dot(gated_out, w_out, preferred_element_type=jnp.float32).astype(jnp.bfloat16)
    return (layer_out, new_state.reshape(BATCH, HEAD, H * VHEAD))
```

```python
import functools

import jax
import jax.numpy as jnp
from jax import lax
from jax.experimental import pallas as pl
from jax.experimental.pallas import tpu as pltpu
from jax.sharding import PartitionSpec as P

HEAD = 256
VHEAD = 512
NEW = 32
EPS = 0.1
SIDE = 4
LANES = 128
TILE = 256


F32 = jnp.float32
BF16 = jnp.bfloat16

ORDER = (0, 1, 3, 2)


def pairs(move):
    out = []
    for y in range(SIDE):
        for x in range(SIDE):
            for c in range(2):
                ty, tx, tc = move(y, x, c)
                out.append(((y * SIDE + x) * 2 + c, (ty * SIDE + tx) * 2 + tc))
    return out


def along(first, step):
    def move(y, x, c):
        return (y ^ step, x, c) if (c == 0) == first else (y, x ^ step, c)

    return pairs(move)


FIRST = {r: along(True, r) for r in (1, 2, 3)}
SECOND = {r: along(False, r) for r in (1, 2, 3)}
OTHER_CORE = pairs(lambda y, x, c: (y, x, 1 - c))


def send(value, table):
    return lax.ppermute(value, "mp", table)


def vmem(count):
    return [pl.BlockSpec(memory_space=pltpu.VMEM)] * count


def params(mib):
    return pltpu.CompilerParams(vmem_limit_bytes=mib * 1024 * 1024)


def project_body(counts, has_sum, last, rows_total, *refs):
    refs = list(refs)
    place = refs.pop(0)
    shards = [refs.pop(0) for _ in counts]
    wq, wqo, wk, wko, wv, wg = (refs.pop(0) for _ in range(6))
    sums = refs.pop(0) if has_sum else None
    outs = refs
    core = place[0]
    half = pl.multiple_of(core * LANES, LANES)
    other_half = pl.multiple_of((1 - core) * LANES, LANES)

    def step(i, carry):
        rows = pl.ds(pl.multiple_of(i * TILE, TILE), TILE)
        pieces = []
        for ref, count in zip(shards, counts):
            if count == 0:
                pieces.append(ref[rows, :])
            else:
                pieces.extend(ref[j, rows, :] for j in range(count))
        left = jnp.concatenate(pieces, axis=1)
        starts = [pl.multiple_of(place[1 + j], LANES) for j in range(len(pieces))]

        def weight(ref):
            return jnp.concatenate([ref[pl.ds(s, LANES), :] for s in starts], axis=0)

        def dot(w):
            return jnp.dot(left, w, preferred_element_type=F32)

        parts = (
            dot(jnp.concatenate([weight(wq), weight(wqo)], axis=1)),
            dot(jnp.concatenate([weight(wk), weight(wko)], axis=1)),
            dot(weight(wv)),
            dot(weight(wg)),
        )
        if has_sum:
            parts = tuple(p + sums[rows, j * 256 : (j + 1) * 256] for j, p in enumerate(parts))
        if not last:
            for j, p in enumerate(parts):
                outs[0][rows, j * 256 : (j + 1) * 256] = p
        else:
            q, k, v, g = parts
            q = (q * HEAD ** (-0.5)).astype(BF16)
            k = k.astype(BF16)
            outs[0][rows, pl.ds(half, LANES)] = q[:, :LANES]
            outs[0][rows, pl.ds(other_half, LANES)] = q[:, LANES:]
            outs[1][rows, pl.ds(half, LANES)] = k[:, :LANES]
            outs[1][rows, pl.ds(other_half, LANES)] = k[:, LANES:]
            outs[2][rows, :] = v.astype(BF16)
            outs[3][rows, :] = g
        return carry

    lax.fori_loop(0, rows_total // TILE, step, 0)


def project(core, shards, chips, weights, sums, last):
    rows = shards[0].shape[-2]
    counts = [0 if s.ndim == 2 else s.shape[0] for s in shards]
    place = jnp.stack([core] + [d * LANES for d in chips]).astype(jnp.int32)
    operands = [place] + shards + list(weights) + ([sums] if sums is not None else [])
    specs = [pl.BlockSpec(memory_space=pltpu.SMEM)] + vmem(len(operands) - 1)
    depth = len(chips) * LANES
    if last:
        shapes = [
            jax.ShapeDtypeStruct((rows, 256), BF16),
            jax.ShapeDtypeStruct((rows, 256), BF16),
            jax.ShapeDtypeStruct((rows, 256), BF16),
            jax.ShapeDtypeStruct((rows, 256), F32),
        ]
    else:
        shapes = [jax.ShapeDtypeStruct((rows, 1024), F32)]
    aliases = {len(operands) - 1: 0} if sums is not None and not last else {}
    return pl.pallas_call(
        functools.partial(project_body, counts, sums is not None, last, rows),
        out_shape=shapes,
        in_specs=specs,
        out_specs=vmem(len(shapes)),
        input_output_aliases=aliases,
        compiler_params=params(24),
        cost_estimate=pl.CostEstimate(
            flops=2 * rows * depth * 1024, bytes_accessed=rows * depth * 2, transcendentals=0
        ),
        name="project_last" if last else "project",
    )(*operands)


def retain_body(q_ref, k_ref, v_ref, col_ref, row_ref, state_ref, out_ref, stat_ref):
    n = lax.broadcasted_iota(jnp.int32, (NEW, NEW), 0)
    m = lax.broadcasted_iota(jnp.int32, (NEW, NEW), 1)
    causal = n >= m

    def step(b, carry):
        rows = pl.ds(pl.multiple_of(b * NEW, NEW), NEW)
        q, k, v = q_ref[rows, :], k_ref[rows, :], v_ref[rows, :]
        col = col_ref[rows, :]
        row = row_ref[pl.ds(b, 1), :]
        from_state = jnp.dot(q, state_ref[b].astype(BF16), preferred_element_type=F32)
        scores = lax.dot_general(q, k, (((1,), (1,)), ((), ())), preferred_element_type=F32)
        gap = jnp.where(causal, col - row, 0.0)
        weights = (scores * jnp.where(causal, jnp.exp(gap), 0.0)).astype(BF16)
        kept = jnp.exp(col) * from_state + jnp.dot(weights, v, preferred_element_type=F32)
        out_ref[rows, :] = kept
        stat_ref[rows, 0:1] = jnp.sum(kept, axis=1, keepdims=True)
        stat_ref[rows, 1:2] = jnp.sum(kept * kept, axis=1, keepdims=True)
        return carry

    lax.fori_loop(0, q_ref.shape[0] // NEW, step, 0, unroll=4)


def retain(q, k, v, col, row, state):
    rows = q.shape[0]
    return pl.pallas_call(
        retain_body,
        out_shape=[jax.ShapeDtypeStruct((rows, 256), F32), jax.ShapeDtypeStruct((rows, 2), F32)],
        in_specs=vmem(6),
        out_specs=vmem(2),
        compiler_params=params(16),
        cost_estimate=pl.CostEstimate(
            flops=2 * rows * 256 * 512, bytes_accessed=state.size * 4, transcendentals=rows * 64
        ),
        name="retain",
    )(q, k, v, col, row, state)


def renew_body(k_ref, v_ref, keep_ref, final_ref, state_ref, out_ref):
    count = state_ref.shape[0]
    for b in range(count):
        rows = slice(b * NEW, (b + 1) * NEW)
        k = (k_ref[rows, :].astype(F32) * keep_ref[rows, :]).astype(BF16)
        fresh = lax.dot_general(k, v_ref[rows, :], (((0,), (0,)), ((), ())), preferred_element_type=F32)
        out_ref[b] = final_ref[b * NEW : b * NEW + 1, :] * state_ref[b] + fresh


def renew(k, v, keep, final, state):
    count = state.shape[0]
    block = 4
    return pl.pallas_call(
        renew_body,
        grid=(count // block,),
        out_shape=jax.ShapeDtypeStruct(state.shape, F32),
        in_specs=[
            pl.BlockSpec((block * NEW, 256), lambda i: (i, 0)),
            pl.BlockSpec((block * NEW, 256), lambda i: (i, 0)),
            pl.BlockSpec((block * NEW, 1), lambda i: (i, 0)),
            pl.BlockSpec((block * NEW, 1), lambda i: (i, 0)),
            pl.BlockSpec((block, 256, 256), lambda i: (i, 0, 0)),
        ],
        out_specs=pl.BlockSpec((block, 256, 256), lambda i: (i, 0, 0)),
        compiler_params=pltpu.CompilerParams(vmem_limit_bytes=16 * 1024 * 1024),
        cost_estimate=pl.CostEstimate(
            flops=8 * 1024 * 1024 * 1024, bytes_accessed=2 * state.size * 4, transcendentals=0
        ),
        name="renew",
    )(k, v, keep, final, state)


def emit_body(place, own_ref, other_ref, w_ref, wo_ref, out_ref):
    def step(i, carry):
        rows = pl.ds(pl.multiple_of(i * TILE, TILE), TILE)
        left = jnp.concatenate([own_ref[rows, :], other_ref[rows, :]], axis=1)
        for j in (0, 2):
            columns = []
            for b in (j, j + 1):
                at = pl.ds(pl.multiple_of(place[b], LANES), LANES)
                columns.append(jnp.concatenate([w_ref[:, at], wo_ref[:, at]], axis=0))
            got = jnp.dot(left, jnp.concatenate(columns, axis=1), preferred_element_type=F32).astype(BF16)
            out_ref[j, rows, :] = got[:, :LANES]
            out_ref[j + 1, rows, :] = got[:, LANES:]
        return carry

    lax.fori_loop(0, own_ref.shape[0] // TILE, step, 0)


def emit(own, other, w, wo, blocks):
    rows = own.shape[0]
    place = jnp.stack([b * LANES for b in blocks]).astype(jnp.int32)
    return pl.pallas_call(
        emit_body,
        out_shape=jax.ShapeDtypeStruct((4, rows, LANES), BF16),
        in_specs=[pl.BlockSpec(memory_space=pltpu.SMEM)] + vmem(4),
        out_specs=pl.BlockSpec(memory_space=pltpu.VMEM),
        compiler_params=params(16),
        cost_estimate=pl.CostEstimate(
            flops=2 * rows * 512 * 512, bytes_accessed=rows * 1024 * 2, transcendentals=0
        ),
        name="emit",
    )(place, own, other, w, wo)


def total(*values):
    out = values[0].astype(F32)
    for v in values[1:]:
        out = out + v.astype(F32)
    return out


def per_device(tokens, decay, state, w_query, w_key, w_value, w_gate, w_out, norm_gain):
    rows = tokens.shape[0]
    sequences = rows // NEW
    me = lax.axis_index("mp")
    core = me % 2
    chip = me // 2
    y, x = chip // SIDE, chip % SIDE
    first = jnp.where(core == 0, y, x)
    second = jnp.where(core == 0, x, y)

    def device(r1, r2, c):
        a, b = first ^ r1, second ^ r2
        return jnp.where(core == 0, a * SIDE + b, b * SIDE + a) * 2 + c

    def other_device(r1, r2):
        a, b = first ^ r2, second ^ r1
        return jnp.where(core == 0, a * SIDE + b, b * SIDE + a) * 2 + 1 - core

    wqo = send(w_query, OTHER_CORE)
    wko = send(w_key, OTHER_CORE)
    weights = (w_query, wqo, w_key, wko, w_value, w_gate)

    s = tokens
    s10, s30 = send(s, FIRST[1]), send(s, FIRST[3])
    s01, s03 = send(s, SECOND[1]), send(s, SECOND[3])
    half = rows // 2
    s20 = jnp.concatenate([send(s30[:half], FIRST[1]), send(s10[half:], FIRST[3])], axis=0)
    s11, s13 = send(s10, SECOND[1]), send(s10, SECOND[3])
    s31, s33 = send(s30, SECOND[1]), send(s30, SECOND[3])
    s21, s23 = send(s20, SECOND[1]), send(s20, SECOND[3])
    s02 = send(s03, SECOND[1])
    s12 = send(s11, SECOND[3])
    s32 = send(s33, SECOND[1])
    s22 = send(s21, SECOND[3])

    groups = (
        (((0, 0), s), ((1, 0), s10), ((3, 0), s30), ((0, 1), s01), ((0, 3), s03)),
        (((2, 0), s20), ((1, 1), s11), ((1, 3), s13), ((3, 1), s31), ((3, 3), s33), ((0, 2), s02)),
        (((2, 1), s21), ((2, 3), s23), ((1, 2), s12), ((3, 2), s32), ((2, 2), s22)),
    )
    sums = None
    for number, group in enumerate(groups):
        shards, devices = [], []
        for (r1, r2), shard in group:
            shards += [shard, send(shard, OTHER_CORE)]
            devices += [device(r1, r2, core), other_device(r1, r2)]
        got = project(core, shards, devices, weights, sums, number == 2)
        sums = got[0]
    query, key_proj, value_proj, gate_proj = got
    w_out_other = send(w_out, OTHER_CORE)

    head = me // 2
    rates = lax.dynamic_slice_in_dim(decay, head, 1, 1).reshape(sequences, NEW)
    log_cumul = jnp.cumsum(jnp.log(rates), axis=1)
    final_log = log_cumul[:, -1:]
    column = log_cumul.reshape(rows, 1)
    keep = jnp.exp(final_log - log_cumul).reshape(rows, 1)
    final = jnp.broadcast_to(jnp.exp(final_log), (sequences, NEW)).reshape(rows, 1)

    retained, stats = retain(query, key_proj, value_proj, column, log_cumul, state)
    stats = stats + send(stats, OTHER_CORE)
    centre = stats[:, 0:1] / VHEAD
    variance = stats[:, 1:2] / VHEAD - centre * centre
    scale = lax.rsqrt(variance + EPS)
    gated = ((retained - centre) * scale * norm_gain * jax.nn.silu(gate_proj)).astype(BF16)
    gated_other = send(gated, OTHER_CORE)

    def blocks(r2):
        return [device(r1, r2, core) for r1 in ORDER]

    g2 = emit(gated, gated_other, w_out, w_out_other, blocks(2))
    g1 = emit(gated, gated_other, w_out, w_out_other, blocks(1))
    g3 = emit(gated, gated_other, w_out, w_out_other, blocks(3))
    g0 = emit(gated, gated_other, w_out, w_out_other, blocks(0))
    new_state = renew(key_proj, value_proj, keep, final, state)

    e1 = send(g2[:2], SECOND[1])
    e3 = send(g2[2:], SECOND[3])
    f1 = send(g1[:2], SECOND[1])
    f3 = send(g3[2:], SECOND[3])
    h1 = send(total(g1[2:], e3).astype(BF16), SECOND[1])
    h3 = send(total(g3[:2], e1).astype(BF16), SECOND[3])
    t01 = total(g0[:2], f1, h3)
    t32 = total(g0[2:], h1, f3)
    t0, t1, t3, t2 = t01[0], t01[1].astype(BF16), t32[0].astype(BF16), t32[1].astype(BF16)
    u2 = send(t2, FIRST[2])
    u1 = send(t1, FIRST[1])
    u3 = send(t3, FIRST[3])
    layer_out = total(t0, u1, u3, u2).astype(BF16)
    return (layer_out, new_state)


def solution(mesh):
    placed = (
        P("dp", "mp"),
        P("dp", None),
        P("dp", None, "mp"),
        P(None, "mp"),
        P(None, "mp"),
        P(None, "mp"),
        P(None, "mp"),
        P("mp", None),
        P("mp"),
    )
    return jax.shard_map(
        per_device,
        mesh=mesh,
        in_specs=placed,
        out_specs=(P("dp", "mp"), P("dp", None, "mp")),
        check_vma=False,
    )
```

```python
import functools

import jax
import jax.numpy as jnp
from jax import lax
from jax.experimental import pallas as pl
from jax.experimental.pallas import tpu as pltpu
from jax.sharding import PartitionSpec as P


HEAD = 256
VHEAD = 512
NEW = 32
EPS = 0.1
SIDE = 4
LANES = 128


F32 = jnp.float32
BF16 = jnp.bfloat16

ORDER = (0, 1, 3, 2)


def pairs(move):
    out = []
    for y in range(SIDE):
        for x in range(SIDE):
            for c in range(2):
                ty, tx, tc = move(y, x, c)
                out.append(((y * SIDE + x) * 2 + c, (ty * SIDE + tx) * 2 + tc))
    return out


def along(first, step):
    def move(y, x, c):
        return (y ^ step, x, c) if (c == 0) == first else (y, x ^ step, c)

    return pairs(move)


FIRST = {r: along(True, r) for r in (1, 2, 3)}
SECOND = {r: along(False, r) for r in (1, 2, 3)}
OTHER_CORE = pairs(lambda y, x, c: (y, x, 1 - c))


def send(value, table):
    return lax.ppermute(value, "mp", table)


def position():
    me = lax.axis_index("mp")
    core = lax.rem(me, 2)
    x = lax.rem(lax.div(me, 2), SIDE)
    y = lax.div(me, 2 * SIDE)
    swap = core * (x - y)
    return core, y + swap, x - swap


def chip_at(core, a, b):
    y, x = a + core * (b - a), b + core * (a - b)
    return y * SIDE + x


def vmem(count):
    return [pl.BlockSpec(memory_space=pltpu.VMEM)] * count


def params(mib):
    return pltpu.CompilerParams(vmem_limit_bytes=mib * 1024 * 1024)


def kernel(body, shapes, operands, mib, flops, **more):
    count = len(shapes)
    more.setdefault("in_specs", vmem(len(operands)))
    more.setdefault("out_specs", vmem(count))
    size = sum(a.size * a.dtype.itemsize for a in operands)
    return pl.pallas_call(
        body,
        out_shape=[jax.ShapeDtypeStruct(*s) for s in shapes],
        compiler_params=params(mib),
        cost_estimate=pl.CostEstimate(flops=int(flops), bytes_accessed=size, transcendentals=0),
        **more,
    )(*operands)


def total(*values):
    out = values[0].astype(F32)
    for v in values[1:]:
        out = out + v.astype(F32)
    return out


def deal_body(own_ref, other_ref, out_ref, sems):
    core, _, _ = position()
    count = out_ref.shape[0]
    rows = pl.ds(pl.multiple_of(core * count, count), count)
    copies = [
        pltpu.make_async_copy(
            ref.at[rows], out_ref.at[:, pl.ds(pl.multiple_of(c * LANES, LANES), LANES)], sems.at[i]
        )
        for i, (ref, c) in enumerate(((own_ref, core), (other_ref, 1 - core)))
    ]
    for c in copies:
        c.start()
    for c in copies:
        c.wait()


def finish_body(a_ref, b_ref, c_ref, u1_ref, u3_ref, u2_ref, mine_ref, theirs_ref):
    core, _, _ = position()
    for out, c in ((mine_ref, core), (theirs_ref, 1 - core)):
        lanes = pl.ds(pl.multiple_of(c * LANES, LANES), LANES)
        out[...] = total(
            a_ref[0, :, lanes],
            b_ref[0, :, lanes],
            *(ref[:, lanes] for ref in (c_ref, u1_ref, u3_ref, u2_ref)),
        ).astype(BF16)


def join_body(mine_ref, theirs_ref, out_ref):
    core, _, _ = position()
    count = mine_ref.shape[0]
    out_ref[pl.ds(pl.multiple_of(core * count, count), count), :] = mine_ref[...]
    out_ref[pl.ds(pl.multiple_of((1 - core) * count, count), count), :] = theirs_ref[...]


def stack_body(a_ref, b_ref, out_ref):
    out_ref[0] = a_ref[...]
    out_ref[1] = b_ref[...]


def add_body(places, *refs):
    refs[-1][...] = total(*(ref[...] if p is None else ref[p] for p, ref in zip(places, refs))).astype(BF16)


def add(*terms):
    arrays = [a for a, _ in terms]
    return kernel(functools.partial(add_body, [p for _, p in terms]), [(arrays[0].shape[-2:], BF16)], arrays, 8, 1e6)[0]


def pick_body(state_ref, out_ref, sems):
    core, _, _ = position()
    count = out_ref.shape[0]
    pieces = 4
    each = count // pieces
    copies = [
        pltpu.make_async_copy(
            state_ref.at[pl.ds((1 - core) * count + i * each, each)],
            out_ref.at[pl.ds(i * each, each)],
            sems.at[i],
        )
        for i in range(pieces)
    ]
    for c in copies:
        c.start()
    for c in copies:
        c.wait()


def project_body(places, count, has_sum, last, *refs):
    refs = list(refs)
    shards = [refs.pop(0) for _ in range(count)]
    wq, wqo, wk, wko, wv, wvo, wg, wgo = (refs.pop(0) for _ in range(8))
    sums = refs.pop(0) if has_sum else None
    outs = refs
    core, first, second = position()
    starts = [pl.multiple_of(chip_at(core, first ^ r1, second ^ r2) * 256, 256) for r1, r2 in places]
    pieces = []
    for ref in shards:
        pieces += [ref[...]] if len(ref.shape) == 2 else [ref[i] for i in range(ref.shape[0])]
    left = jnp.concatenate(pieces, axis=1)

    def weight(ref):
        return jnp.concatenate([ref[pl.ds(s, 256), :] for s in starts], axis=0)

    def dot(j, *ws):
        w = jnp.concatenate([weight(r) for r in ws], axis=1) if len(ws) > 1 else weight(ws[0])
        out = jnp.dot(left, w, preferred_element_type=F32)
        return out + sums[:, j * 256 : (j + 1) * 256] if has_sum else out

    columns = ((wq, wqo), (wk, wko), (wv,), (wvo,), (wg,), (wgo,))
    for j, ws in enumerate(columns):
        got = dot(j, *ws)
        if not last:
            outs[0][:, j * 256 : (j + 1) * 256] = got
        elif j < 2:
            if j == 0:
                got = got * HEAD ** (-0.5)
            got = got.astype(BF16)
            outs[j][:, pl.ds(pl.multiple_of(core * LANES, LANES), LANES)] = got[:, :LANES]
            outs[j][:, pl.ds(pl.multiple_of((1 - core) * LANES, LANES), LANES)] = got[:, LANES:]
        elif j < 4:
            outs[j][...] = got.astype(BF16)
        else:
            outs[j][...] = got


def project(places, shards, weights, sums, last):
    rows = shards[0].shape[-2]
    operands = list(shards) + list(weights) + ([sums] if sums is not None else [])
    if last:
        shapes = [((rows, 256), BF16)] * 4 + [((rows, 256), F32)] * 2
    else:
        shapes = [((rows, 1536), F32)]
    aliases = {len(operands) - 1: 0} if sums is not None and not last else {}
    return kernel(
        functools.partial(project_body, places, len(shards), sums is not None, last),
        shapes,
        operands,
        12,
        2 * rows * 256 * len(places) * 1536,
        input_output_aliases=aliases,
    )


def decay_body(decay_ref, col_ref, row_ref):
    head = lax.div(lax.axis_index("mp"), 2)
    step = 8 * NEW
    line = lax.broadcasted_iota(jnp.int32, (decay_ref.shape[0], step), 0)
    r = lax.broadcasted_iota(jnp.int32, (step, step), 0)
    m = lax.broadcasted_iota(jnp.int32, (step, step), 1)
    before = jnp.where((r // NEW == m // NEW) & (m <= r), 1.0, 0.0)
    token = lax.broadcasted_iota(jnp.int32, (step, NEW), 0) % NEW
    upto = jnp.where(token <= lax.broadcasted_iota(jnp.int32, (step, NEW), 1), 1.0, 0.0)
    owner = lax.broadcasted_iota(jnp.int32, (8, step), 1) // NEW == lax.broadcasted_iota(jnp.int32, (8, step), 0)
    for i in range(decay_ref.shape[1] // step):
        at = slice(i * step, (i + 1) * step)
        rate = jnp.sum(jnp.where(line == head, decay_ref[:, at], 0.0), axis=0, keepdims=True)
        logs = jnp.broadcast_to(jnp.log(rate), (8, step))
        col_ref[at, :] = lax.dot_general(
            before, logs, (((1,), (1,)), ((), ())), precision=lax.Precision.HIGHEST, preferred_element_type=F32
        )[:, :1]
        row_ref[i * 8 : (i + 1) * 8, :] = jnp.dot(
            jnp.where(owner, logs, 0.0), upto, precision=lax.Precision.HIGHEST, preferred_element_type=F32
        )


def retain_body(
    q_ref, k_ref, v_ref, vo_ref, g_ref, go_ref, col_ref, row_ref, state_ref, other_ref, gain_ref, gaino_ref, out_ref
):
    core, _, _ = position()
    n = lax.broadcasted_iota(jnp.int32, (NEW, NEW), 0)
    m = lax.broadcasted_iota(jnp.int32, (NEW, NEW), 1)
    causal = n >= m
    count = other_ref.shape[0]
    gains = (gain_ref[...], gaino_ref[...])

    def group(first, number):
        rows = [pl.ds(pl.multiple_of((first + b) * NEW, NEW), NEW) for b in range(number)]
        seqs = [core * count + first + b for b in range(number)]
        q = [q_ref[r, :] for r in rows]
        scores = [
            lax.dot_general(a, k_ref[r, :], (((1,), (1,)), ((), ())), preferred_element_type=F32)
            for a, r in zip(q, rows)
        ]
        cols = [col_ref[pl.ds(pl.multiple_of(s * NEW, NEW), NEW), :] for s in seqs]
        old = [
            [jnp.dot(a, ref[at].astype(BF16), preferred_element_type=F32) for ref, at in ((state_ref, s), (other_ref, first + b))]
            for b, (a, s) in enumerate(zip(q, seqs))
        ]
        weights = [
            (x * jnp.where(causal, jnp.exp(jnp.where(causal, c - row_ref[pl.ds(s, 1), :], 0.0)), 0.0)).astype(BF16)
            for x, c, s in zip(scores, cols, seqs)
        ]
        new = [[jnp.dot(w, v[r, :], preferred_element_type=F32) for v in (v_ref, vo_ref)] for w, r in zip(weights, rows)]
        kept = [[jnp.exp(c) * a + b for a, b in zip(o, n)] for c, o, n in zip(cols, old, new)]
        centres = [sum(jnp.sum(p, axis=1, keepdims=True) for p in k) / VHEAD for k in kept]
        kept = [[p - c for p in k] for k, c in zip(kept, centres)]
        scales = [
            lax.rsqrt(sum(jnp.sum(p * p, axis=1, keepdims=True) for p in k) / VHEAD + EPS) for k in kept
        ]
        for r, k, scale in zip(rows, kept, scales):
            for j, (p, g, gain) in enumerate(zip(k, (g_ref, go_ref), gains)):
                gate = g[r, :]
                out_ref[r, j * 256 : (j + 1) * 256] = (
                    p * scale * gain * (gate / (1.0 + jnp.exp(-gate)))
                ).astype(BF16)

    number = 8

    def step(i, carry):
        group(i * number, number)
        return carry

    lax.fori_loop(0, count // number, step, 0)


def renew_body(start, k_ref, ko_ref, v_ref, vo_ref, col_ref, state_ref, *rest):
    out_ref = rest[-1]
    core, _, _ = position()
    count = out_ref.shape[0]
    block = pl.program_id(0) * count
    half = k_ref.shape[0] // NEW
    mine = core == start // half
    for b in range(count):
        seq = start + block + b
        rows = pl.ds(pl.multiple_of((block + b) * NEW, NEW), NEW)
        col = col_ref[pl.ds(pl.multiple_of(seq * NEW, NEW), NEW), :]
        last = col[NEW - 1 : NEW, :]
        k = jnp.where(mine, k_ref[rows, :], ko_ref[rows, :])
        v = jnp.where(mine, v_ref[rows, :], vo_ref[rows, :])
        k = (k.astype(F32) * jnp.exp(last - col)).astype(BF16)
        fresh = lax.dot_general(k, v, (((0,), (0,)), ((), ())), preferred_element_type=F32)
        out_ref[b] = jnp.exp(last) * state_ref[seq] + fresh


def renew(operands, start, count, old=None):
    block = 4
    state = operands[-1]
    extra = [old] if old is not None else []
    return kernel(
        functools.partial(renew_body, start),
        [(state.shape, F32)],
        list(operands) + extra,
        8,
        2e9,
        grid=(count // block,),
        in_specs=vmem(len(operands)) + [pl.BlockSpec(memory_space=pl.ANY)] * len(extra),
        out_specs=[pl.BlockSpec((block, 256, 256), lambda i: (i + start // block, 0, 0))],
        input_output_aliases={len(operands): 0} if extra else {},
    )[0]


def emit_body(r2, gated_ref, w_ref, wo_ref, *outs):
    core, first, second = position()
    left = gated_ref[...]
    for j, r1 in enumerate(ORDER):
        at = pl.ds(pl.multiple_of(chip_at(core, first ^ r1, second ^ r2) * 256, 256), 256)
        w = jnp.concatenate([w_ref[:, at], wo_ref[:, at]], axis=0)
        outs[j // 2][j % 2] = jnp.dot(left, w, preferred_element_type=F32).astype(BF16)


def per_device(tokens, decay, state, w_query, w_key, w_value, w_gate, w_out, norm_gain):
    rows = tokens.shape[0] // 2
    sequences = rows // NEW

    px = send(tokens, OTHER_CORE)
    (s,) = kernel(
        deal_body,
        [((rows, 256), BF16)],
        [tokens, px],
        8,
        1e6,
        in_specs=[pl.BlockSpec(memory_space=pl.ANY)] * 2,
        scratch_shapes=[pltpu.SemaphoreType.DMA((2,))],
    )
    s10, s30, s20 = send(s, FIRST[1]), send(s, FIRST[3]), send(s, FIRST[2])
    s03, s01 = send(s, SECOND[3]), send(s, SECOND[1])
    (near,) = kernel(stack_body, [((2, rows, 256), BF16)], [s10, s30], 8, 1e6)
    near1, near3 = send(near, SECOND[1]), send(near, SECOND[3])
    s21, s23 = send(s20, SECOND[1]), send(s20, SECOND[3])
    s02 = send(s03, SECOND[1])
    near2 = send(near1, SECOND[3])
    s22 = send(s23, SECOND[1])

    weights = []
    for w in (w_query, w_key, w_value, w_gate):
        weights += [w, send(w, OTHER_CORE)]
    (away,) = kernel(
        pick_body,
        [((sequences, 256, 256), F32)],
        [state],
        8,
        1e6,
        in_specs=[pl.BlockSpec(memory_space=pl.ANY)],
        scratch_shapes=[pltpu.SemaphoreType.DMA((4,))],
    )
    state_other = send(away, OTHER_CORE)
    gain = norm_gain.reshape(1, 256)
    gain_other = send(gain, OTHER_CORE)
    w_other = send(w_out, OTHER_CORE)
    column, row = kernel(decay_body, [((2 * rows, 1), F32), ((2 * sequences, NEW), F32)], [decay.T], 8, 8e9)

    groups = (
        ("project_a", (s, s10, s30, s20, s01, s03), ((0, 0), (1, 0), (3, 0), (2, 0), (0, 1), (0, 3))),
        ("project_b", (near1, near3, s21, s23, s02), ((1, 1), (3, 1), (1, 3), (3, 3), (2, 1), (2, 3), (0, 2))),
        ("project_c", (near2, s22), ((1, 2), (3, 2), (2, 2))),
    )
    sums = None
    for name, shards, places in groups:
        got = project(places, shards, weights, sums, name == "project_c")
        sums = got[0]
    query, key, value, value_other, gate, gate_other = got

    (gated,) = kernel(
        retain_body,
        [((rows, 512), BF16)],
        [query, key, value, value_other, gate, gate_other, column, row, state, state_other, gain, gain_other],
        8,
        2 * rows * 512 * 512,
    )

    g = {}
    for r2 in (2, 1, 3, 0):
        g[r2] = kernel(
            functools.partial(emit_body, r2),
            [((2, rows, 256), BF16)] * 2,
            [gated, w_out, w_other],
            8,
            2 * rows * 512 * 1024,
        )

    fresh = (key, send(key, OTHER_CORE), value, send(value_other, OTHER_CORE), column, state)
    new_state = renew(fresh, 0, sequences)
    new_state = renew(fresh, sequences, sequences, new_state)

    e1 = send(g[2][0], SECOND[1])
    e3 = send(g[2][1], SECOND[3])
    f1 = send(g[1][0], SECOND[1])
    f3 = send(g[3][1], SECOND[3])
    h12 = send(total(g[1][1][1], e3[1]).astype(BF16), SECOND[1])
    h31 = send(total(g[3][0][1], e1[1]).astype(BF16), SECOND[3])
    h13 = send(total(g[1][1][0], e3[0]).astype(BF16), SECOND[1])
    h30 = send(total(g[3][0][0], e1[0]).astype(BF16), SECOND[3])
    u2 = send(add((g[0][1], 1), (h12, None), (f3, 1)), FIRST[2])
    u1 = send(add((g[0][0], 1), (f1, 1), (h31, None)), FIRST[1])
    u3 = send(add((g[0][1], 0), (h13, None), (f3, 0)), FIRST[3])
    mine, theirs = kernel(finish_body, [((rows, LANES), BF16)] * 2, [g[0][0], f1, h30, u1, u3, u2], 8, 1e6)
    (layer_out,) = kernel(join_body, [((2 * rows, LANES), BF16)], [mine, send(theirs, OTHER_CORE)], 8, 1e6)
    return (layer_out, new_state)


def solution(mesh):
    placed = (
        P("dp", "mp"),
        P("dp", None),
        P("dp", None, "mp"),
        P(None, "mp"),
        P(None, "mp"),
        P(None, "mp"),
        P(None, "mp"),
        P("mp", None),
        P("mp"),
    )

    return jax.shard_map(
        per_device,
        mesh=mesh,
        in_specs=placed,
        out_specs=(P("dp", "mp"), P("dp", None, "mp")),
        check_vma=False,
    )
```

```python
import functools

import jax
import jax.numpy as jnp
from jax import lax
from jax.experimental import pallas as pl
from jax.experimental.pallas import tpu as pltpu
from jax.sharding import PartitionSpec as P


HEAD = 256
VHEAD = 512
NEW = 32
EPS = 0.1
SIDE = 4
LANES = 128


F32 = jnp.float32
BF16 = jnp.bfloat16

ORDER = (0, 1, 3, 2)


def pairs(move):
    out = []
    for y in range(SIDE):
        for x in range(SIDE):
            for c in range(2):
                ty, tx, tc = move(y, x, c)
                out.append(((y * SIDE + x) * 2 + c, (ty * SIDE + tx) * 2 + tc))
    return out


def along(first, step):
    def move(y, x, c):
        return (y ^ step, x, c) if (c == 0) == first else (y, x ^ step, c)

    return pairs(move)


FIRST = {r: along(True, r) for r in (1, 2, 3)}
SECOND = {r: along(False, r) for r in (1, 2, 3)}
OTHER_CORE = pairs(lambda y, x, c: (y, x, 1 - c))


def send(value, table):
    return lax.ppermute(value, "mp", table)


def position():
    me = lax.axis_index("mp")
    core = lax.rem(me, 2)
    x = lax.rem(lax.div(me, 2), SIDE)
    y = lax.div(me, 2 * SIDE)
    swap = core * (x - y)
    return core, y + swap, x - swap


def chip_at(core, a, b):
    y, x = a + core * (b - a), b + core * (a - b)
    return y * SIDE + x


def vmem(count):
    return [pl.BlockSpec(memory_space=pltpu.VMEM)] * count


def params(mib):
    return pltpu.CompilerParams(vmem_limit_bytes=mib * 1024 * 1024)


def kernel(body, shapes, operands, mib, flops, **more):
    count = len(shapes)
    more.setdefault("in_specs", vmem(len(operands)))
    more.setdefault("out_specs", vmem(count))
    size = sum(a.size * a.dtype.itemsize for a in operands)
    return pl.pallas_call(
        body,
        out_shape=[jax.ShapeDtypeStruct(*s) for s in shapes],
        compiler_params=params(mib),
        cost_estimate=pl.CostEstimate(flops=int(flops), bytes_accessed=size, transcendentals=0),
        **more,
    )(*operands)


def total(*values):
    out = values[0].astype(F32)
    for v in values[1:]:
        out = out + v.astype(F32)
    return out


def own_body(ref, out_ref):
    core, _, _ = position()
    count = out_ref.shape[0]
    out_ref[...] = ref[pl.ds(pl.multiple_of(core * count, count), count), :]


def deal_body(own_ref, other_ref, out_ref):
    core, _, _ = position()
    count = out_ref.shape[0]
    rows = pl.ds(pl.multiple_of(core * count, count), count)
    out_ref[:, pl.ds(pl.multiple_of(core * LANES, LANES), LANES)] = own_ref[...]
    out_ref[:, pl.ds(pl.multiple_of((1 - core) * LANES, LANES), LANES)] = other_ref[rows, :]


def finish_body(a_ref, b_ref, c_ref, u1_ref, u3_ref, u2_ref, mine_ref, theirs_ref):
    core, _, _ = position()
    for out, c in ((mine_ref, core), (theirs_ref, 1 - core)):
        lanes = pl.ds(pl.multiple_of(c * LANES, LANES), LANES)
        out[...] = total(
            a_ref[0, :, lanes],
            b_ref[0, :, lanes],
            *(ref[:, lanes] for ref in (c_ref, u1_ref, u3_ref, u2_ref)),
        ).astype(BF16)


def join_body(mine_ref, theirs_ref, out_ref):
    core, _, _ = position()
    count = mine_ref.shape[0]
    out_ref[pl.ds(pl.multiple_of(core * count, count), count), :] = mine_ref[...]
    out_ref[pl.ds(pl.multiple_of((1 - core) * count, count), count), :] = theirs_ref[...]


def stack_body(a_ref, b_ref, out_ref):
    out_ref[0] = a_ref[...]
    out_ref[1] = b_ref[...]


def add_body(places, *refs):
    refs[-1][...] = total(*(ref[...] if p is None else ref[p] for p, ref in zip(places, refs))).astype(BF16)


def add(*terms):
    arrays = [a for a, _ in terms]
    return kernel(functools.partial(add_body, [p for _, p in terms]), [(arrays[0].shape[-2:], BF16)], arrays, 8, 1e6)[0]


def pick_body(state_ref, out_ref, sems):
    core, _, _ = position()
    count = out_ref.shape[0]
    pieces = 4
    each = count // pieces
    copies = [
        pltpu.make_async_copy(
            state_ref.at[pl.ds((1 - core) * count + i * each, each)],
            out_ref.at[pl.ds(i * each, each)],
            sems.at[i],
        )
        for i in range(pieces)
    ]
    for c in copies:
        c.start()
    for c in copies:
        c.wait()


def project_body(places, count, has_sum, last, *refs):
    refs = list(refs)
    shards = [refs.pop(0) for _ in range(count)]
    wq, wqo, wk, wko, wv, wvo, wg, wgo = (refs.pop(0) for _ in range(8))
    sums = refs.pop(0) if has_sum else None
    outs = refs
    core, first, second = position()
    starts = [pl.multiple_of(chip_at(core, first ^ r1, second ^ r2) * 256, 256) for r1, r2 in places]
    pieces = []
    for ref in shards:
        pieces += [ref[...]] if len(ref.shape) == 2 else [ref[i] for i in range(ref.shape[0])]
    left = jnp.concatenate(pieces, axis=1)

    def weight(ref):
        return jnp.concatenate([ref[pl.ds(s, 256), :] for s in starts], axis=0)

    def dot(j, *ws):
        w = jnp.concatenate([weight(r) for r in ws], axis=1) if len(ws) > 1 else weight(ws[0])
        out = jnp.dot(left, w, preferred_element_type=F32)
        return out + sums[:, j * 256 : (j + 1) * 256] if has_sum else out

    columns = ((wq, wqo), (wk, wko), (wv,), (wvo,), (wg,), (wgo,))
    for j, ws in enumerate(columns):
        got = dot(j, *ws)
        if not last:
            outs[0][:, j * 256 : (j + 1) * 256] = got
        elif j < 2:
            if j == 0:
                got = got * HEAD ** (-0.5)
            got = got.astype(BF16)
            outs[j][:, pl.ds(pl.multiple_of(core * LANES, LANES), LANES)] = got[:, :LANES]
            outs[j][:, pl.ds(pl.multiple_of((1 - core) * LANES, LANES), LANES)] = got[:, LANES:]
        elif j < 4:
            outs[j][...] = got.astype(BF16)
        else:
            outs[j][...] = got


def project(places, shards, weights, sums, last):
    rows = shards[0].shape[-2]
    operands = list(shards) + list(weights) + ([sums] if sums is not None else [])
    if last:
        shapes = [((rows, 256), BF16)] * 4 + [((rows, 256), F32)] * 2
    else:
        shapes = [((rows, 1536), F32)]
    aliases = {len(operands) - 1: 0} if sums is not None and not last else {}
    return kernel(
        functools.partial(project_body, places, len(shards), sums is not None, last),
        shapes,
        operands,
        12,
        2 * rows * 256 * len(places) * 1536,
        input_output_aliases=aliases,
    )


def decay_body(decay_ref, col_ref, row_ref):
    head = lax.div(lax.axis_index("mp"), 2)
    step = 8 * NEW
    line = lax.broadcasted_iota(jnp.int32, (decay_ref.shape[0], step), 0)
    r = lax.broadcasted_iota(jnp.int32, (step, step), 0)
    m = lax.broadcasted_iota(jnp.int32, (step, step), 1)
    before = jnp.where((r // NEW == m // NEW) & (m <= r), 1.0, 0.0)
    token = lax.broadcasted_iota(jnp.int32, (step, NEW), 0) % NEW
    upto = jnp.where(token <= lax.broadcasted_iota(jnp.int32, (step, NEW), 1), 1.0, 0.0)
    owner = lax.broadcasted_iota(jnp.int32, (8, step), 1) // NEW == lax.broadcasted_iota(jnp.int32, (8, step), 0)
    for i in range(decay_ref.shape[1] // step):
        at = slice(i * step, (i + 1) * step)
        rate = jnp.sum(jnp.where(line == head, decay_ref[:, at], 0.0), axis=0, keepdims=True)
        logs = jnp.broadcast_to(jnp.log(rate), (8, step))
        col_ref[at, :] = lax.dot_general(
            before, logs, (((1,), (1,)), ((), ())), precision=lax.Precision.HIGHEST, preferred_element_type=F32
        )[:, :1]
        row_ref[i * 8 : (i + 1) * 8, :] = jnp.dot(
            jnp.where(owner, logs, 0.0), upto, precision=lax.Precision.HIGHEST, preferred_element_type=F32
        )


def retain_body(
    q_ref, k_ref, v_ref, vo_ref, g_ref, go_ref, col_ref, row_ref, state_ref, other_ref, gain_ref, gaino_ref, out_ref
):
    core, _, _ = position()
    n = lax.broadcasted_iota(jnp.int32, (NEW, NEW), 0)
    m = lax.broadcasted_iota(jnp.int32, (NEW, NEW), 1)
    causal = n >= m
    count = other_ref.shape[0]
    gains = (gain_ref[...], gaino_ref[...])

    def group(first, number):
        rows = [pl.ds(pl.multiple_of((first + b) * NEW, NEW), NEW) for b in range(number)]
        seqs = [core * count + first + b for b in range(number)]
        q = [q_ref[r, :] for r in rows]
        scores = [
            lax.dot_general(a, k_ref[r, :], (((1,), (1,)), ((), ())), preferred_element_type=F32)
            for a, r in zip(q, rows)
        ]
        cols = [col_ref[pl.ds(pl.multiple_of(s * NEW, NEW), NEW), :] for s in seqs]
        old = [
            [jnp.dot(a, ref[at].astype(BF16), preferred_element_type=F32) for ref, at in ((state_ref, s), (other_ref, first + b))]
            for b, (a, s) in enumerate(zip(q, seqs))
        ]
        weights = [
            (x * jnp.where(causal, jnp.exp(jnp.where(causal, c - row_ref[pl.ds(s, 1), :], 0.0)), 0.0)).astype(BF16)
            for x, c, s in zip(scores, cols, seqs)
        ]
        new = [[jnp.dot(w, v[r, :], preferred_element_type=F32) for v in (v_ref, vo_ref)] for w, r in zip(weights, rows)]
        kept = [[jnp.exp(c) * a + b for a, b in zip(o, n)] for c, o, n in zip(cols, old, new)]
        centres = [sum(jnp.sum(p, axis=1, keepdims=True) for p in k) / VHEAD for k in kept]
        kept = [[p - c for p in k] for k, c in zip(kept, centres)]
        scales = [
            lax.rsqrt(sum(jnp.sum(p * p, axis=1, keepdims=True) for p in k) / VHEAD + EPS) for k in kept
        ]
        for r, k, scale in zip(rows, kept, scales):
            for j, (p, g, gain) in enumerate(zip(k, (g_ref, go_ref), gains)):
                gate = g[r, :]
                out_ref[r, j * 256 : (j + 1) * 256] = (
                    p * scale * gain * (gate / (1.0 + jnp.exp(-gate)))
                ).astype(BF16)

    number = 8

    def step(i, carry):
        group(i * number, number)
        return carry

    lax.fori_loop(0, count // number, step, 0)


def renew_body(start, k_ref, ko_ref, v_ref, vo_ref, col_ref, state_ref, *rest):
    out_ref = rest[-1]
    core, _, _ = position()
    count = out_ref.shape[0]
    block = pl.program_id(0) * count
    half = k_ref.shape[0] // NEW
    mine = core == start // half
    inside = start % half + block
    for b in range(count):
        seq = start + block + b
        rows = pl.ds(pl.multiple_of((inside + b) * NEW, NEW), NEW)
        col = col_ref[pl.ds(pl.multiple_of(seq * NEW, NEW), NEW), :]
        last = col[NEW - 1 : NEW, :]
        k = jnp.where(mine, k_ref[rows, :], ko_ref[rows, :])
        v = jnp.where(mine, v_ref[rows, :], vo_ref[rows, :])
        k = (k.astype(F32) * jnp.exp(last - col)).astype(BF16)
        fresh = lax.dot_general(k, v, (((0,), (0,)), ((), ())), preferred_element_type=F32)
        out_ref[b] = jnp.exp(last) * state_ref[seq] + fresh


def renew(operands, start, count, old=None):
    block = 4
    state = operands[-1]
    extra = [old] if old is not None else []
    return kernel(
        functools.partial(renew_body, start),
        [(state.shape, F32)],
        list(operands) + extra,
        8,
        1e9,
        grid=(count // block,),
        in_specs=vmem(len(operands)) + [pl.BlockSpec(memory_space=pl.ANY)] * len(extra),
        out_specs=[pl.BlockSpec((block, 256, 256), lambda i: (i + start // block, 0, 0))],
        input_output_aliases={len(operands): 0} if extra else {},
    )[0]


def emit_body(r2, gated_ref, w_ref, wo_ref, *outs):
    core, first, second = position()
    left = gated_ref[...]
    for j, r1 in enumerate(ORDER):
        at = pl.ds(pl.multiple_of(chip_at(core, first ^ r1, second ^ r2) * 256, 256), 256)
        w = jnp.concatenate([w_ref[:, at], wo_ref[:, at]], axis=0)
        outs[j // 2][j % 2] = jnp.dot(left, w, preferred_element_type=F32).astype(BF16)


def per_device(tokens, decay, state, w_query, w_key, w_value, w_gate, w_out, norm_gain):
    rows = tokens.shape[0] // 2
    sequences = rows // NEW

    px = send(tokens, OTHER_CORE)
    (own,) = kernel(own_body, [((rows, LANES), BF16)], [tokens], 8, 1e6)
    (s,) = kernel(deal_body, [((rows, 256), BF16)], [own, px], 8, 1e6)
    s10, s30, s20 = send(s, FIRST[1]), send(s, FIRST[3]), send(s, FIRST[2])
    s03, s01 = send(s, SECOND[3]), send(s, SECOND[1])
    (near,) = kernel(stack_body, [((2, rows, 256), BF16)], [s10, s30], 8, 1e6)
    near1, near3 = send(near, SECOND[1]), send(near, SECOND[3])
    s21, s23 = send(s20, SECOND[1]), send(s20, SECOND[3])
    s02 = send(s03, SECOND[1])
    near2 = send(near1, SECOND[3])
    s22 = send(s23, SECOND[1])

    weights = []
    for w in (w_query, w_key, w_value, w_gate):
        weights += [w, send(w, OTHER_CORE)]
    (away,) = kernel(
        pick_body,
        [((sequences, 256, 256), F32)],
        [state],
        8,
        1e6,
        in_specs=[pl.BlockSpec(memory_space=pl.ANY)],
        scratch_shapes=[pltpu.SemaphoreType.DMA((4,))],
    )
    state_other = send(away, OTHER_CORE)
    gain = norm_gain.reshape(1, 256)
    gain_other = send(gain, OTHER_CORE)
    w_other = send(w_out, OTHER_CORE)
    column, row = kernel(decay_body, [((2 * rows, 1), F32), ((2 * sequences, NEW), F32)], [decay.T], 8, 8e9)

    groups = (
        ("project_a", (s, s10, s30, s20), ((0, 0), (1, 0), (3, 0), (2, 0))),
        (
            "project_b",
            (s01, s03, near1, near3, s21, s23, s02),
            ((0, 1), (0, 3), (1, 1), (3, 1), (1, 3), (3, 3), (2, 1), (2, 3), (0, 2)),
        ),
        ("project_c", (near2, s22), ((1, 2), (3, 2), (2, 2))),
    )
    sums = None
    for name, shards, places in groups:
        got = project(places, shards, weights, sums, name == "project_c")
        sums = got[0]
    query, key, value, value_other, gate, gate_other = got

    (gated,) = kernel(
        retain_body,
        [((rows, 512), BF16)],
        [query, key, value, value_other, gate, gate_other, column, row, state, state_other, gain, gain_other],
        8,
        2 * rows * 512 * 512,
    )

    g = {}
    for r2 in (2, 1, 3, 0):
        g[r2] = kernel(
            functools.partial(emit_body, r2),
            [((2, rows, 256), BF16)] * 2,
            [gated, w_out, w_other],
            8,
            2 * rows * 512 * 1024,
        )

    fresh = (key, send(key, OTHER_CORE), value, send(value_other, OTHER_CORE), column, state)
    new_state, part = None, sequences // 2
    for number in range(4):
        new_state = renew(fresh, number * part, part, new_state)

    e1 = send(g[2][0], SECOND[1])
    e3 = send(g[2][1], SECOND[3])
    f1 = send(g[1][0], SECOND[1])
    f3 = send(g[3][1], SECOND[3])
    h12 = send(total(g[1][1][1], e3[1]).astype(BF16), SECOND[1])
    h31 = send(total(g[3][0][1], e1[1]).astype(BF16), SECOND[3])
    h13 = send(total(g[1][1][0], e3[0]).astype(BF16), SECOND[1])
    h30 = send(total(g[3][0][0], e1[0]).astype(BF16), SECOND[3])
    u2 = send(add((g[0][1], 1), (h12, None), (f3, 1)), FIRST[2])
    u1 = send(add((g[0][0], 1), (f1, 1), (h31, None)), FIRST[1])
    u3 = send(add((g[0][1], 0), (h13, None), (f3, 0)), FIRST[3])
    mine, theirs = kernel(finish_body, [((rows, LANES), BF16)] * 2, [g[0][0], f1, h30, u1, u3, u2], 8, 1e6)
    (layer_out,) = kernel(join_body, [((2 * rows, LANES), BF16)], [mine, send(theirs, OTHER_CORE)], 8, 1e6)
    return (layer_out, new_state)


def solution(mesh):
    placed = (
        P("dp", "mp"),
        P("dp", None),
        P("dp", None, "mp"),
        P(None, "mp"),
        P(None, "mp"),
        P(None, "mp"),
        P(None, "mp"),
        P("mp", None),
        P("mp"),
    )

    return jax.shard_map(
        per_device,
        mesh=mesh,
        in_specs=placed,
        out_specs=(P("dp", "mp"), P("dp", None, "mp")),
        check_vma=False,
    )
```

```python
import functools

import jax
import jax.numpy as jnp
from jax import lax
from jax.experimental import pallas as pl
from jax.experimental.pallas import tpu as pltpu
from jax.sharding import PartitionSpec as P


HEAD = 256
VHEAD = 512
NEW = 32
EPS = 0.1
SIDE = 4
LANES = 128


F32 = jnp.float32
BF16 = jnp.bfloat16

ORDER = (0, 1, 3, 2)


def pairs(move):
    out = []
    for y in range(SIDE):
        for x in range(SIDE):
            for c in range(2):
                ty, tx, tc = move(y, x, c)
                out.append(((y * SIDE + x) * 2 + c, (ty * SIDE + tx) * 2 + tc))
    return out


def along(first, step):
    def move(y, x, c):
        return (y ^ step, x, c) if (c == 0) == first else (y, x ^ step, c)

    return pairs(move)


FIRST = {r: along(True, r) for r in (1, 2, 3)}
SECOND = {r: along(False, r) for r in (1, 2, 3)}
OTHER_CORE = pairs(lambda y, x, c: (y, x, 1 - c))


def send(value, table):
    return lax.ppermute(value, "mp", table)


def position():
    me = lax.axis_index("mp")
    core = lax.rem(me, 2)
    x = lax.rem(lax.div(me, 2), SIDE)
    y = lax.div(me, 2 * SIDE)
    swap = core * (x - y)
    return core, y + swap, x - swap


def chip_at(core, a, b):
    y, x = a + core * (b - a), b + core * (a - b)
    return y * SIDE + x


def vmem(count):
    return [pl.BlockSpec(memory_space=pltpu.VMEM)] * count


def params(mib):
    return pltpu.CompilerParams(vmem_limit_bytes=mib * 1024 * 1024)


def kernel(body, shapes, operands, mib, flops, **more):
    count = len(shapes)
    more.setdefault("in_specs", vmem(len(operands)))
    more.setdefault("out_specs", vmem(count))
    size = sum(a.size * a.dtype.itemsize for a in operands)
    return pl.pallas_call(
        body,
        out_shape=[jax.ShapeDtypeStruct(*s) for s in shapes],
        compiler_params=params(mib),
        cost_estimate=pl.CostEstimate(flops=int(flops), bytes_accessed=size, transcendentals=0),
        **more,
    )(*operands)


def total(*values):
    out = values[0].astype(F32)
    for v in values[1:]:
        out = out + v.astype(F32)
    return out


def own_body(ref, out_ref):
    core, _, _ = position()
    count = out_ref.shape[0]
    out_ref[...] = ref[pl.ds(pl.multiple_of(core * count, count), count), :]


def deal_body(own_ref, other_ref, out_ref):
    core, _, _ = position()
    count = out_ref.shape[0]
    rows = pl.ds(pl.multiple_of(core * count, count), count)
    out_ref[:, pl.ds(pl.multiple_of(core * LANES, LANES), LANES)] = own_ref[...]
    out_ref[:, pl.ds(pl.multiple_of((1 - core) * LANES, LANES), LANES)] = other_ref[rows, :]


def finish_body(a_ref, b_ref, c_ref, u1_ref, u3_ref, u2_ref, mine_ref, theirs_ref):
    core, _, _ = position()
    for out, c in ((mine_ref, core), (theirs_ref, 1 - core)):
        lanes = pl.ds(pl.multiple_of(c * LANES, LANES), LANES)
        out[...] = total(
            a_ref[0, :, lanes],
            b_ref[0, :, lanes],
            *(ref[:, lanes] for ref in (c_ref, u1_ref, u3_ref, u2_ref)),
        ).astype(BF16)


def join_body(mine_ref, theirs_ref, out_ref):
    core, _, _ = position()
    count = mine_ref.shape[0]
    out_ref[pl.ds(pl.multiple_of(core * count, count), count), :] = mine_ref[...]
    out_ref[pl.ds(pl.multiple_of((1 - core) * count, count), count), :] = theirs_ref[...]


def stack_body(a_ref, b_ref, out_ref):
    out_ref[0] = a_ref[...]
    out_ref[1] = b_ref[...]


def add_body(places, *refs):
    refs[-1][...] = total(*(ref[...] if p is None else ref[p] for p, ref in zip(places, refs))).astype(BF16)


def add(*terms):
    arrays = [a for a, _ in terms]
    return kernel(functools.partial(add_body, [p for _, p in terms]), [(arrays[0].shape[-2:], BF16)], arrays, 8, 1e6)[0]


def pick_body(state_ref, out_ref, sems):
    core, _, _ = position()
    count = out_ref.shape[0]
    pieces = 4
    each = count // pieces
    copies = [
        pltpu.make_async_copy(
            state_ref.at[pl.ds((1 - core) * count + i * each, each)],
            out_ref.at[pl.ds(i * each, each)],
            sems.at[i],
        )
        for i in range(pieces)
    ]
    for c in copies:
        c.start()
    for c in copies:
        c.wait()


def project_body(places, count, has_sum, last, *refs):
    refs = list(refs)
    shards = [refs.pop(0) for _ in range(count)]
    wq, wqo, wk, wko, wv, wvo, wg, wgo = (refs.pop(0) for _ in range(8))
    sums = refs.pop(0) if has_sum else None
    outs = refs
    core, first, second = position()
    starts = [pl.multiple_of(chip_at(core, first ^ r1, second ^ r2) * 256, 256) for r1, r2 in places]
    pieces = []
    for ref in shards:
        pieces += [ref[...]] if len(ref.shape) == 2 else [ref[i] for i in range(ref.shape[0])]
    left = jnp.concatenate(pieces, axis=1)

    def weight(ref):
        return jnp.concatenate([ref[pl.ds(s, 256), :] for s in starts], axis=0)

    def dot(j, *ws):
        w = jnp.concatenate([weight(r) for r in ws], axis=1) if len(ws) > 1 else weight(ws[0])
        out = jnp.dot(left, w, preferred_element_type=F32)
        return out + sums[:, j * 256 : (j + 1) * 256] if has_sum else out

    columns = ((wq, wqo), (wk, wko), (wv,), (wvo,), (wg,), (wgo,))
    for j, ws in enumerate(columns):
        got = dot(j, *ws)
        if not last:
            outs[0][:, j * 256 : (j + 1) * 256] = got
        elif j < 2:
            if j == 0:
                got = got * HEAD ** (-0.5)
            got = got.astype(BF16)
            outs[j][:, pl.ds(pl.multiple_of(core * LANES, LANES), LANES)] = got[:, :LANES]
            outs[j][:, pl.ds(pl.multiple_of((1 - core) * LANES, LANES), LANES)] = got[:, LANES:]
        elif j < 4:
            outs[j][...] = got.astype(BF16)
        else:
            outs[j][...] = got


def project(places, shards, weights, sums, last):
    rows = shards[0].shape[-2]
    operands = list(shards) + list(weights) + ([sums] if sums is not None else [])
    if last:
        shapes = [((rows, 256), BF16)] * 4 + [((rows, 256), F32)] * 2
    else:
        shapes = [((rows, 1536), F32)]
    aliases = {len(operands) - 1: 0} if sums is not None and not last else {}
    return kernel(
        functools.partial(project_body, places, len(shards), sums is not None, last),
        shapes,
        operands,
        12,
        2 * rows * 256 * len(places) * 1536,
        input_output_aliases=aliases,
    )


def decay_body(decay_ref, col_ref, row_ref):
    head = lax.div(lax.axis_index("mp"), 2)
    step = 8 * NEW
    line = lax.broadcasted_iota(jnp.int32, (decay_ref.shape[0], step), 0)
    r = lax.broadcasted_iota(jnp.int32, (step, step), 0)
    m = lax.broadcasted_iota(jnp.int32, (step, step), 1)
    before = jnp.where((r // NEW == m // NEW) & (m <= r), 1.0, 0.0)
    token = lax.broadcasted_iota(jnp.int32, (step, NEW), 0) % NEW
    upto = jnp.where(token <= lax.broadcasted_iota(jnp.int32, (step, NEW), 1), 1.0, 0.0)
    owner = lax.broadcasted_iota(jnp.int32, (8, step), 1) // NEW == lax.broadcasted_iota(jnp.int32, (8, step), 0)
    for i in range(decay_ref.shape[1] // step):
        at = slice(i * step, (i + 1) * step)
        rate = jnp.sum(jnp.where(line == head, decay_ref[:, at], 0.0), axis=0, keepdims=True)
        logs = jnp.broadcast_to(jnp.log(rate), (8, step))
        col_ref[at, :] = lax.dot_general(
            before, logs, (((1,), (1,)), ((), ())), precision=lax.Precision.HIGHEST, preferred_element_type=F32
        )[:, :1]
        row_ref[i * 8 : (i + 1) * 8, :] = jnp.dot(
            jnp.where(owner, logs, 0.0), upto, precision=lax.Precision.HIGHEST, preferred_element_type=F32
        )


def retain_body(
    q_ref, k_ref, v_ref, vo_ref, g_ref, go_ref, col_ref, row_ref, state_ref, other_ref, gain_ref, gaino_ref, out_ref
):
    core, _, _ = position()
    n = lax.broadcasted_iota(jnp.int32, (NEW, NEW), 0)
    m = lax.broadcasted_iota(jnp.int32, (NEW, NEW), 1)
    causal = n >= m
    count = other_ref.shape[0]
    gains = (gain_ref[...], gaino_ref[...])

    def group(first, number):
        rows = [pl.ds(pl.multiple_of((first + b) * NEW, NEW), NEW) for b in range(number)]
        seqs = [core * count + first + b for b in range(number)]
        q = [q_ref[r, :] for r in rows]
        scores = [
            lax.dot_general(a, k_ref[r, :], (((1,), (1,)), ((), ())), preferred_element_type=F32)
            for a, r in zip(q, rows)
        ]
        cols = [col_ref[pl.ds(pl.multiple_of(s * NEW, NEW), NEW), :] for s in seqs]
        old = [
            [jnp.dot(a, ref[at].astype(BF16), preferred_element_type=F32) for ref, at in ((state_ref, s), (other_ref, first + b))]
            for b, (a, s) in enumerate(zip(q, seqs))
        ]
        weights = [
            (x * jnp.where(causal, jnp.exp(jnp.where(causal, c - row_ref[pl.ds(s, 1), :], 0.0)), 0.0)).astype(BF16)
            for x, c, s in zip(scores, cols, seqs)
        ]
        new = [[jnp.dot(w, v[r, :], preferred_element_type=F32) for v in (v_ref, vo_ref)] for w, r in zip(weights, rows)]
        kept = [[jnp.exp(c) * a + b for a, b in zip(o, n)] for c, o, n in zip(cols, old, new)]
        centres = [sum(jnp.sum(p, axis=1, keepdims=True) for p in k) / VHEAD for k in kept]
        kept = [[p - c for p in k] for k, c in zip(kept, centres)]
        scales = [
            lax.rsqrt(sum(jnp.sum(p * p, axis=1, keepdims=True) for p in k) / VHEAD + EPS) for k in kept
        ]
        for r, k, scale in zip(rows, kept, scales):
            for j, (p, g, gain) in enumerate(zip(k, (g_ref, go_ref), gains)):
                gate = g[r, :]
                out_ref[r, j * 256 : (j + 1) * 256] = (
                    p * scale * gain * (gate / (1.0 + jnp.exp(-gate)))
                ).astype(BF16)

    number = 8

    def step(i, carry):
        group(i * number, number)
        return carry

    lax.fori_loop(0, count // number, step, 0)


def renew_body(start, k_ref, ko_ref, v_ref, vo_ref, col_ref, state_ref, *rest):
    out_ref = rest[-1]
    core, _, _ = position()
    count = out_ref.shape[0]
    block = pl.program_id(0) * count
    half = k_ref.shape[0] // NEW
    mine = core == start // half
    inside = start % half + block
    for b in range(count):
        seq = start + block + b
        rows = pl.ds(pl.multiple_of((inside + b) * NEW, NEW), NEW)
        col = col_ref[pl.ds(pl.multiple_of(seq * NEW, NEW), NEW), :]
        last = col[NEW - 1 : NEW, :]
        k = jnp.where(mine, k_ref[rows, :], ko_ref[rows, :])
        v = jnp.where(mine, v_ref[rows, :], vo_ref[rows, :])
        k = (k.astype(F32) * jnp.exp(last - col)).astype(BF16)
        fresh = lax.dot_general(k, v, (((0,), (0,)), ((), ())), preferred_element_type=F32)
        out_ref[b] = jnp.exp(last) * state_ref[seq] + fresh


def renew(operands, start, count, old=None):
    block = 4
    state = operands[-1]
    extra = [old] if old is not None else []
    return kernel(
        functools.partial(renew_body, start),
        [(state.shape, F32)],
        list(operands) + extra,
        8,
        1e9,
        grid=(count // block,),
        in_specs=vmem(len(operands)) + [pl.BlockSpec(memory_space=pl.ANY)] * len(extra),
        out_specs=[pl.BlockSpec((block, 256, 256), lambda i: (i + start // block, 0, 0))],
        input_output_aliases={len(operands): 0} if extra else {},
    )[0]


def emit_body(r2, order, gated_ref, w_ref, wo_ref, *outs):
    core, first, second = position()
    left = gated_ref[...]
    for j, r1 in enumerate(order):
        at = pl.ds(pl.multiple_of(chip_at(core, first ^ r1, second ^ r2) * 256, 256), 256)
        w = jnp.concatenate([w_ref[:, at], wo_ref[:, at]], axis=0)
        outs[j // 2][j % 2] = jnp.dot(left, w, preferred_element_type=F32).astype(BF16)


def per_device(tokens, decay, state, w_query, w_key, w_value, w_gate, w_out, norm_gain):
    rows = tokens.shape[0] // 2
    sequences = rows // NEW

    px = send(tokens, OTHER_CORE)
    (own,) = kernel(own_body, [((rows, LANES), BF16)], [tokens], 8, 1e6)
    (s,) = kernel(deal_body, [((rows, 256), BF16)], [own, px], 8, 1e6)
    s10, s30, s20 = send(s, FIRST[1]), send(s, FIRST[3]), send(s, FIRST[2])
    s03, s01 = send(s, SECOND[3]), send(s, SECOND[1])
    (near,) = kernel(stack_body, [((2, rows, 256), BF16)], [s10, s30], 8, 1e6)
    near1, near3 = send(near, SECOND[1]), send(near, SECOND[3])
    s21, s23 = send(s20, SECOND[1]), send(s20, SECOND[3])
    s02 = send(s03, SECOND[1])
    near2 = send(near1, SECOND[3])
    s22 = send(s23, SECOND[1])

    weights = []
    for w in (w_query, w_key, w_value, w_gate):
        weights += [w, send(w, OTHER_CORE)]
    (away,) = kernel(
        pick_body,
        [((sequences, 256, 256), F32)],
        [state],
        8,
        1e6,
        in_specs=[pl.BlockSpec(memory_space=pl.ANY)],
        scratch_shapes=[pltpu.SemaphoreType.DMA((4,))],
    )
    state_other = send(away, OTHER_CORE)
    gain = norm_gain.reshape(1, 256)
    gain_other = send(gain, OTHER_CORE)
    w_other = send(w_out, OTHER_CORE)
    column, row = kernel(decay_body, [((2 * rows, 1), F32), ((2 * sequences, NEW), F32)], [decay.T], 8, 8e9)

    groups = (
        ("project_a", (s, s10, s30, s20), ((0, 0), (1, 0), (3, 0), (2, 0))),
        (
            "project_b",
            (s01, s03, near1, near3, s21, s23, s02),
            ((0, 1), (0, 3), (1, 1), (3, 1), (1, 3), (3, 3), (2, 1), (2, 3), (0, 2)),
        ),
        ("project_c", (near2,), ((1, 2), (3, 2))),
        ("project_d", (s22,), ((2, 2),)),
    )
    sums = None
    for name, shards, places in groups:
        got = project(places, shards, weights, sums, name == "project_d")
        sums = got[0]
    query, key, value, value_other, gate, gate_other = got

    (gated,) = kernel(
        retain_body,
        [((rows, 512), BF16)],
        [query, key, value, value_other, gate, gate_other, column, row, state, state_other, gain, gain_other],
        8,
        2 * rows * 512 * 512,
    )

    def emit(r2, order):
        return kernel(
            functools.partial(emit_body, r2, order),
            [((2, rows, 256), BF16)] * (len(order) // 2),
            [gated, w_out, w_other],
            8,
            2 * rows * 512 * 256 * len(order),
        )

    g = {2: emit(2, ORDER[:2]) + emit(2, ORDER[2:])}
    for r2 in (1, 3, 0):
        g[r2] = emit(r2, ORDER)

    fresh = (key, send(key, OTHER_CORE), value, send(value_other, OTHER_CORE), column, state)
    new_state, part = None, sequences // 2
    for number in range(4):
        new_state = renew(fresh, number * part, part, new_state)

    e1 = send(g[2][0], SECOND[1])
    e3 = send(g[2][1], SECOND[3])
    f1 = send(g[1][0], SECOND[1])
    f3 = send(g[3][1], SECOND[3])
    h12 = send(total(g[1][1][1], e3[1]).astype(BF16), SECOND[1])
    h31 = send(total(g[3][0][1], e1[1]).astype(BF16), SECOND[3])
    h13 = send(total(g[1][1][0], e3[0]).astype(BF16), SECOND[1])
    h30 = send(total(g[3][0][0], e1[0]).astype(BF16), SECOND[3])
    u2 = send(add((g[0][1], 1), (h12, None), (f3, 1)), FIRST[2])
    u1 = send(add((g[0][0], 1), (f1, 1), (h31, None)), FIRST[1])
    u3 = send(add((g[0][1], 0), (h13, None), (f3, 0)), FIRST[3])
    mine, theirs = kernel(finish_body, [((rows, LANES), BF16)] * 2, [g[0][0], f1, h30, u1, u3, u2], 8, 1e6)
    (layer_out,) = kernel(join_body, [((2 * rows, LANES), BF16)], [mine, send(theirs, OTHER_CORE)], 8, 1e6)
    return (layer_out, new_state)


def solution(mesh):
    placed = (
        P("dp", "mp"),
        P("dp", None),
        P("dp", None, "mp"),
        P(None, "mp"),
        P(None, "mp"),
        P(None, "mp"),
        P(None, "mp"),
        P("mp", None),
        P("mp"),
    )

    return jax.shard_map(
        per_device,
        mesh=mesh,
        in_specs=placed,
        out_specs=(P("dp", "mp"), P("dp", None, "mp")),
        check_vma=False,
    )
```
